32 devices in a mesh: groups: 2 (over y), expert: 8 (over z, x), sub: 2 (over core).
Axes of the slice: x: 2, y: 2, z: 4, core: 2. Of those that a mesh axis runs over, the one named last changes fastest.
Arguments:
- stream_in: bfloat16 [1024, 3072], P(('groups', 'expert'), 'sub'), parts along dimension 0, may hold values from -0.29882812 to 0.29882812
- queries: bfloat16 [1024, 3072], P(('groups', 'expert'), 'sub'), parts along dimension 0, may hold values from -6 to 6
- kv_new: bfloat16 [2, 1024, 1024], P(None, ('groups', 'expert'), 'sub'), parts along dimension 1, may hold values from -6 to 6
- paged_key_value_cache: bfloat16 [2, 32, 4, 1024], P(None, ('groups', 'expert'), None, 'sub'), parts along dimension 1, may hold values from -6 to 6
- page_table: int32 [16, 8], P(('groups', 'expert')), parts along dimension 0, may hold values from 0 to 15, as said below
- prefix_len: int32 [16], P(('groups', 'expert')), parts along dimension 0, may hold values from 8 to 32
- norm_gain: float32 [3072], replicated, may hold values from 0.5 to 1.5
- w_router: bfloat16 [3072, 8], replicated, may hold values from -0.21875 to 0.21875
- expert_ids: int32 [1024, 2], P(('groups', 'expert')), parts along dimension 0, may hold values from 0 to 7, as said below
- w_in: bfloat16 [2, 3072, 65536], P(None, None, ('expert', 'sub')), may hold values from -0.109375 to 0.109375
Outputs:
- stream: bfloat16 [1024, 3072], P(('groups', 'expert'), 'sub'), parts along dimension 0
- expert_hidden: bfloat16 [272, 65536], P('groups', ('expert', 'sub')), parts along dimension 0
The draws below stay inside these ranges and needn't reach their ends.
There are 2 independent parts, one for each index of `groups`. The reference program is written for one: setup_inputs(seed, part) draws one part's arguments, and reference() takes and returns one part's arrays. A program takes and returns all parts, laid end to end along the dimension named above; an argument that names none is the same for every part. Nothing has to cross between parts.
Inputs may be any that keep to these rules, and one draw needn't show every extreme that they name: `expert_ids`: each row names two different experts. The rows of one request name each expert at most 17 times, and one expert is named exactly 17 times by the rows of every request. `page_table`: the pages of one row lie in different shards: page // 2 differs along a row. Requests share leading pages.
All inputs are finite; a program needn't handle non-finite values.
Results may differ from the reference program's by a relative error of at most 0.018.
Values may be sent and summed in bfloat16 or wider, within the bound.
A program may use at most 128 MiB of HBM per device.

```python
import math
import jax
import jax.numpy as jnp
from jax import lax

D = 3072
QUERY_HEADS = 24
KEY_VALUE_HEADS = 8
HEAD_WIDTH = 128
EXPERTS = 8
FF = 8192
TOP = 2
TOK_DEV = 64
PAGE_TOKENS = 4
CP = 2
REQUEST_COUNT = 8
TABLE_PAGES = 8
CACHE_PAGES = 16
SUFFIX_TOKENS = 512
CAP = 17
GROUP = 1
SLOTS = 136
N_EXPERT = 8


def draw_page_table(key, part):
    family_count = max(REQUEST_COUNT // 4, 1)
    joined_keys = jax.random.split(key, 4)
    family_shift = jax.random.randint(joined_keys[0], (family_count,), 0, TABLE_PAGES)
    shared_len = jax.random.randint(joined_keys[1], (REQUEST_COUNT,), 0, TABLE_PAGES + 1)
    family_pages = jax.random.randint(joined_keys[2], (family_count, TABLE_PAGES), 0, CP)
    own_pages = jax.random.randint(joined_keys[3], (REQUEST_COUNT, TABLE_PAGES), 0, CP)
    family_of = jnp.minimum(jnp.arange(REQUEST_COUNT) // 4, family_count - 1)
    column = jnp.arange(TABLE_PAGES)[None, :]
    inside = jnp.where(column < shared_len[:, None], family_pages[family_of], own_pages)
    owner_dev = (column + family_shift[family_of][:, None]) % TABLE_PAGES
    return (owner_dev * CP + inside).astype(jnp.int32)


def draw_prefix_len(key, part):
    joined_keys = jax.random.split(key, 2)
    lengths = jax.random.randint(joined_keys[0], (REQUEST_COUNT,), PAGE_TOKENS * TABLE_PAGES // 4, PAGE_TOKENS * TABLE_PAGES + 1)
    longest = jax.random.randint(joined_keys[1], (), 0, REQUEST_COUNT)
    return jnp.where(jnp.arange(REQUEST_COUNT) == longest, PAGE_TOKENS * TABLE_PAGES, lengths).astype(jnp.int32)


def draw_queries(key, part):
    root_random_key = jax.random.fold_in(key, 11)
    value_rows = jnp.clip(jax.random.normal(root_random_key, (SUFFIX_TOKENS, QUERY_HEADS * HEAD_WIDTH), jnp.float32), -6.0, 6.0)
    return value_rows.astype(jnp.bfloat16)


def draw_kv_new(key, part):
    root_random_key = jax.random.fold_in(key, 13)
    value_rows = jnp.clip(jax.random.normal(root_random_key, (2, SUFFIX_TOKENS, KEY_VALUE_HEADS * HEAD_WIDTH), jnp.float32), -6.0, 6.0)
    return value_rows.astype(jnp.bfloat16)


def shuffled(one_key):
    return jax.random.permutation(one_key, TOK_DEV)


def unit_order(one_key):
    return jax.random.permutation(one_key, (EXPERTS - 1) * CAP)


def draw_expert_ids(key, part):
    joined_keys = jax.random.split(jax.random.fold_in(key, 17), 4)
    hot_expert = jax.random.randint(joined_keys[0], (), 0, EXPERTS)
    remaining = TOK_DEV * TOP - CAP
    units = jax.vmap(unit_order)(jax.random.split(joined_keys[1], REQUEST_COUNT))
    picked = units[:, :remaining] // CAP
    other_counts = jnp.sum((picked[:, :, None] == jnp.arange(EXPERTS - 1)[None, None, :]).astype(jnp.int32), axis=1)
    expert_range = jnp.arange(EXPERTS)
    offset = (expert_range - hot_expert - 1) % EXPERTS
    counts = jnp.where(expert_range[None, :] == hot_expert, CAP, jnp.take(other_counts, jnp.minimum(offset, EXPERTS - 2), axis=1))
    route_ends = jnp.cumsum(counts, axis=1)
    route_pos = jnp.arange(TOK_DEV * TOP)
    sequence = jnp.sum((route_pos[None, :, None] >= route_ends[:, None, :]).astype(jnp.int32), axis=2)
    pair_ids = jnp.stack([sequence[:, :TOK_DEV], sequence[:, TOK_DEV:]], axis=2)
    flip_bits = jax.random.randint(joined_keys[2], (REQUEST_COUNT, TOK_DEV, 1), 0, 2)
    pair_ids = jnp.where(flip_bits == 1, pair_ids[:, :, ::-1], pair_ids)
    orders = jax.vmap(shuffled)(jax.random.split(joined_keys[3], REQUEST_COUNT))
    pair_ids = jnp.take_along_axis(pair_ids, orders[:, :, None], axis=1)
    return pair_ids.reshape(SUFFIX_TOKENS, TOP).astype(jnp.int32)


def levels(stream_key, extent, cuts, least, top_value):
    def one(dim, blocks):
        steps = jax.random.uniform(jax.random.fold_in(jax.random.fold_in(stream_key, 6), dim), (blocks,), jnp.float32, least / len(cuts), top_value / len(cuts))
        return jnp.repeat(jnp.exp(steps), extent[dim] // blocks).reshape((-1,) + (1,) * (len(extent) - dim - 1))

    loudness = one(*cuts[0])
    for cut in cuts[1:]:
        loudness = loudness * one(*cut)
    return loudness


def bell_draw(stream_key, shape, deviation, reach, pieces=(), kind=jnp.bfloat16):
    result = jax.random.normal(stream_key, shape, jnp.float32) * deviation
    if len(pieces) > 0:
        result = levels(stream_key, shape, pieces, -0.22, 0.18) * result
    return jnp.clip(result, min=-reach, max=reach).astype(kind)


def setup_inputs(seed: int = 0, part: int = 0) -> dict:
    splits = jax.random.split(jax.random.key(seed), 11)
    part_keys = jax.random.split(jax.random.fold_in(splits[10], part), 11)
    return {
        "stream_in": bell_draw(part_keys[0], (SUFFIX_TOKENS, D), 0.05, 0.29882812, ((0, 8), (1, 2))),
        "queries": draw_queries(jax.random.fold_in(jax.random.fold_in(splits[10], part), 71), part),
        "kv_new": draw_kv_new(jax.random.fold_in(jax.random.fold_in(splits[10], part), 71), part),
        "paged_key_value_cache": bell_draw(part_keys[3], (2, CACHE_PAGES, PAGE_TOKENS, KEY_VALUE_HEADS * HEAD_WIDTH), 1.0, 6.0, ((1, 8), (3, 2))),
        "page_table": draw_page_table(jax.random.fold_in(jax.random.fold_in(splits[10], part), 71), part),
        "prefix_len": draw_prefix_len(jax.random.fold_in(jax.random.fold_in(splits[10], part), 71), part),
        "norm_gain": jnp.clip(1.0 + 0.1 * jax.random.normal(splits[6], (D,), jnp.float32), 0.5, 1.5),
        "w_router": bell_draw(splits[7], (D, EXPERTS), (D // 4) ** -0.5, 0.21875),
        "expert_ids": draw_expert_ids(jax.random.fold_in(jax.random.fold_in(splits[10], part), 71), part),
        "w_in": bell_draw(splits[9], (2, D, EXPERTS * FF), D ** -0.5, 0.109375, ((2, 16),)),
    }


def attend(query_rows, key_rows, prefix_length, head_size):
    tokens_here = query_rows.shape[0]
    length = key_rows.shape[1]
    kv_heads = key_rows.shape[2] // head_size
    grouped = query_rows.shape[1] // head_size // kv_heads
    query_f = query_rows.reshape(tokens_here, kv_heads, grouped, head_size).astype(jnp.float32)
    keys_f = key_rows[0].reshape(length, kv_heads, head_size).astype(jnp.float32)
    values_f = key_rows[1].reshape(length, kv_heads, head_size).astype(jnp.float32)
    scores = jnp.einsum('tkgd,lkd->kgtl', query_f, keys_f) * (1.0 / math.sqrt(head_size))
    prefix_span = length - tokens_here
    places = jnp.arange(length)[None, :]
    rows_at = jnp.arange(tokens_here)[:, None]
    is_live = jnp.where(places < prefix_span, places < prefix_length, places - prefix_span <= rows_at)
    scores = jnp.where(is_live, scores, -1e+30)
    largest = lax.optimization_barrier(jnp.max(scores, axis=-1, keepdims=True))
    exponent = jnp.exp(scores - largest)
    weights = (exponent / lax.optimization_barrier(jnp.sum(exponent, axis=-1, keepdims=True))).astype(jnp.bfloat16)
    mixed_heads = jnp.einsum('kgtl,lkd->tkgd', weights.astype(jnp.float32), values_f)
    return mixed_heads.reshape(tokens_here, -1).astype(jnp.bfloat16)

def reference(stream_in, queries, kv_new, paged_key_value_cache, page_table, prefix_len, norm_gain, w_router, expert_ids, w_in):

    def one_request(request):
        page_list = page_table[request]
        page_row_block = jnp.take(paged_key_value_cache, page_list, axis=1)
        prefix_row_block = page_row_block.reshape(2, TABLE_PAGES * PAGE_TOKENS, KEY_VALUE_HEADS * HEAD_WIDTH)
        row_start = (request * TOK_DEV).astype(jnp.int32)
        suffix = lax.dynamic_slice_in_dim(kv_new, row_start, TOK_DEV, 1)
        query_rows = lax.dynamic_slice_in_dim(queries, row_start, TOK_DEV, 0)
        key_rows = jnp.concatenate([prefix_row_block, suffix], axis=1)
        return attend(query_rows, key_rows, prefix_len[request], HEAD_WIDTH)
    attended = lax.map(one_request, jnp.arange(REQUEST_COUNT, dtype=jnp.int32)).reshape(SUFFIX_TOKENS, QUERY_HEADS * HEAD_WIDTH)
    stream = (stream_in.astype(jnp.float32) + attended.astype(jnp.float32)).astype(jnp.bfloat16)
    stream_f = stream.astype(jnp.float32)
    scale_rows = lax.rsqrt(lax.optimization_barrier(jnp.mean(stream_f * stream_f, axis=-1, keepdims=True)) + 1e-05)
    normed = (stream_f * scale_rows * norm_gain).astype(jnp.bfloat16)
    logits = jnp.dot(normed, w_router, preferred_element_type=jnp.float32)
    chosen = jnp.take_along_axis(logits, expert_ids, axis=1)
    gate_share = jax.nn.sigmoid(chosen - chosen[:, ::-1])
    route_ids = expert_ids.reshape(N_EXPERT, TOK_DEV * TOP)
    expert_hot = (route_ids[:, :, None] == jnp.arange(EXPERTS, dtype=jnp.int32)[None, None, :]).astype(jnp.int32)
    route_rank = lax.optimization_barrier(jnp.sum((jnp.cumsum(expert_hot, axis=1) - 1) * expert_hot, axis=2)).astype(jnp.int32)
    request_ids = jnp.arange(N_EXPERT, dtype=jnp.int32)
    slot_base = ((request_ids % GROUP * EXPERTS + request_ids // GROUP) * CAP).astype(jnp.int32)
    slot_at = (slot_base[:, None] + route_rank).astype(jnp.int32)
    token_at = (request_ids[:, None] * TOK_DEV + jnp.arange(TOK_DEV * TOP, dtype=jnp.int32)[None, :] // TOP).astype(jnp.int32)
    token_slots = jnp.zeros((EXPERTS, SLOTS), jnp.int32).at[route_ids, slot_at].set(token_at)
    share_flat = gate_share.reshape(N_EXPERT, TOK_DEV * TOP)
    slot_shares = jnp.zeros((EXPERTS, SLOTS), jnp.float32).at[route_ids, slot_at].set(share_flat)
    columns = []
    for expert in range(EXPERTS):
        slot_rows = jnp.take(normed, token_slots[expert], axis=0)
        gate_part = jnp.dot(slot_rows, w_in[0, :, expert * FF:(expert + 1) * FF], preferred_element_type=jnp.float32)
        up_part = jnp.dot(slot_rows, w_in[1, :, expert * FF:(expert + 1) * FF], preferred_element_type=jnp.float32)
        columns.append((jax.nn.silu(gate_part) * up_part * slot_shares[expert][:, None]).astype(jnp.bfloat16))
    return (stream, jnp.concatenate(columns, axis=1))
```

```python
import math

import jax
import jax.numpy as jnp
from jax import lax
from jax.experimental import pallas as pl
from jax.experimental.pallas import tpu as pltpu
from jax.sharding import PartitionSpec as P

HEAD_WIDTH = 128
EXPERTS = 8
CAP = 17
MAIN = 16
LANES = 128
F32 = jnp.float32
BF16 = jnp.bfloat16
MESH = pl.DeviceIdType.MESH


def dot(a, b):
    return jnp.dot(a, b, preferred_element_type=F32)


def iota(shape, dim):
    return lax.broadcasted_iota(jnp.int32, shape, dim)


def kernel(
    count,
    w_chunks,
    page_tokens,
    page_table,
    prefix_len,
    stream_in,
    queries,
    kv_new,
    cache,
    norm_gain,
    w_router,
    expert_ids,
    w_in,
    stream_out,
    hidden_out,
    weights,
    kv_all,
    part,
    part_in,
    rows_out,
    last_out,
    rows_in,
    last_in,
    rows_over,
    last_over,
    slots,
    w_sem,
    page_send,
    page_recv,
    part_send,
    part_recv,
    row_send,
    row_recv,
    last_send,
    last_recv,
    over_send,
    over_recv,
    over_last_send,
    over_last_recv,
):
    me = lax.axis_index("expert")
    core = lax.axis_index("sub")
    width = count // EXPERTS
    half = stream_in.shape[1]
    tokens = stream_in.shape[0]
    holder = me // width

    def place(index):
        return (index % width) * EXPERTS + index // width

    barrier = pltpu.get_barrier_semaphore()

    def greet(step, carry):
        pl.semaphore_signal(
            barrier, inc=1, device_id={"expert": (me + step) % count}, device_id_type=MESH
        )
        return carry

    lax.fori_loop(1, count, greet, 0)
    pl.semaphore_signal(barrier, inc=1, device_id={"sub": 1 - core}, device_id_type=MESH)

    depth = weights.shape[1] // w_chunks
    loads = []
    for chunk in range(w_chunks):
        for side in range(2):
            span = pl.ds(chunk * depth, depth)
            load = pltpu.make_async_copy(
                w_in.at[side, span], weights.at[side, span], w_sem.at[side, chunk]
            )
            load.start()
            loads.append(load)

    pl.semaphore_wait(barrier, count)

    def page_copy(step):
        return pltpu.make_async_remote_copy(
            src_ref=cache,
            dst_ref=kv_all.at[me],
            send_sem=page_send.at[step],
            recv_sem=page_recv.at[step],
            device_id={"expert": (me + step) % count},
            device_id_type=MESH,
        )

    def start_pages(step, carry):
        page_copy(step).start()
        return carry

    lax.fori_loop(1, count, start_pages, 0)
    kv_all[me] = cache[...]

    shard_rows = cache.shape[1]
    page_rows = kv_all.shape[0] * shard_rows
    table_pages = page_table.shape[1]
    tokens_page = page_tokens
    key_heads = kv_new.shape[2] // HEAD_WIDTH
    grouped = half // HEAD_WIDTH // key_heads
    scaling = 1.0 / math.sqrt(HEAD_WIDTH)
    flat = ((1,), (1,)), ((), ())
    stacked = tokens * grouped
    causal = iota((stacked, tokens), 1) <= iota((stacked, tokens), 0) % tokens
    asked = []
    own_scores = []
    for head in range(key_heads):
        lanes = slice(head * HEAD_WIDTH, (head + 1) * HEAD_WIDTH)
        query = jnp.concatenate(
            [
                queries[:, (head * grouped + g) * HEAD_WIDTH : (head * grouped + g + 1) * HEAD_WIDTH]
                for g in range(grouped)
            ],
            axis=0,
        )
        asked.append(query)
        score = lax.dot_general(query, kv_new[0, :, lanes], flat, preferred_element_type=F32)
        own_scores.append(jnp.where(causal, score * scaling, -1e30))

    row_at = iota((1, page_rows), 1)
    page_at = row_at // tokens_page

    def find(j, found):
        return jnp.where(page_at == page_table[0, j], j * tokens_page, found)

    never = jnp.full((1, page_rows), 1 << 29, jnp.int32)
    position = lax.fori_loop(0, table_pages, find, never) + row_at % tokens_page
    alive = position < prefix_len[0]

    def wait_pages(step, carry):
        page_copy(step).wait()
        return carry

    lax.fori_loop(1, count, wait_pages, 0)

    for head in range(key_heads):
        lanes = slice(head * HEAD_WIDTH, (head + 1) * HEAD_WIDTH)
        keys = kv_all[:, 0, :, lanes].astype(F32).reshape(page_rows, HEAD_WIDTH).astype(BF16)
        values = kv_all[:, 1, :, lanes].astype(F32).reshape(page_rows, HEAD_WIDTH).astype(BF16)
        old = lax.dot_general(asked[head], keys, flat, preferred_element_type=F32) * scaling
        old = jnp.where(alive, old, -1e30)
        new = own_scores[head]
        largest = jnp.maximum(
            jnp.max(old, axis=1, keepdims=True), jnp.max(new, axis=1, keepdims=True)
        )
        old = jnp.exp(old - largest)
        new = jnp.exp(new - largest)
        total = jnp.sum(old, axis=1, keepdims=True) + jnp.sum(new, axis=1, keepdims=True)
        mixed = dot((old / total).astype(BF16), values)
        mixed = mixed + dot((new / total).astype(BF16), kv_new[1, :, lanes])
        mixed = mixed.astype(BF16).astype(F32)
        for g in range(grouped):
            at = slice((head * grouped + g) * HEAD_WIDTH, (head * grouped + g + 1) * HEAD_WIDTH)
            stream_out[:, at] = (
                stream_in[:, at].astype(F32) + mixed[g * tokens : (g + 1) * tokens]
            ).astype(BF16)

    stream = stream_out[...].astype(F32)
    first = pl.multiple_of(core * half, LANES)
    gain = norm_gain[:, pl.ds(first, half)]
    squares = jnp.sum(stream * stream, axis=1, keepdims=True)
    raw = dot((stream * gain).astype(BF16), w_router[pl.ds(first, half), :])
    part[0] = jnp.zeros((tokens, LANES), F32)
    part[0, :, 0:EXPERTS] = raw
    part[1] = jnp.broadcast_to(squares, (tokens, LANES))
    swap = pltpu.make_async_remote_copy(
        src_ref=part,
        dst_ref=part_in,
        send_sem=part_send,
        recv_sem=part_recv,
        device_id={"sub": 1 - core},
        device_id_type=MESH,
    )
    swap.start()

    lane = iota((tokens, LANES), 1)
    named = (expert_ids[:, 0:1] == lane) | (expert_ids[:, 1:2] == lane)
    hot = named.astype(F32)
    hot_b = hot.astype(BF16)
    before = (iota((tokens, tokens), 0) < iota((tokens, tokens), 1)).astype(F32).astype(BF16)
    same = (iota((tokens, tokens), 0) == iota((tokens, tokens), 1)).astype(F32).astype(BF16)
    turn = ((0,), (0,)), ((), ())
    rank = lax.dot_general(hot_b, before, turn, preferred_element_type=F32)[0:EXPERTS]
    is_hot = lax.dot_general(hot_b, same, turn, preferred_element_type=F32)[0:EXPERTS]
    rank = jnp.where(is_hot > 0.5, rank, -1.0)
    slot = iota((MAIN, tokens), 0).astype(F32)
    picker = jnp.concatenate(
        [
            (jnp.broadcast_to(rank[e : e + 1], (MAIN, tokens)) == slot).astype(F32)
            for e in range(EXPERTS)
        ],
        axis=0,
    ).astype(BF16)
    last_picker = (rank == float(MAIN)).astype(F32).astype(BF16)

    swap.wait()
    scale = lax.rsqrt((part[1] + part_in[1])[:, 0:1] / (2 * half) + 1e-05)
    logits = (part[0] + part_in[0]) * scale
    chosen = logits * hot
    both = jnp.sum(chosen, axis=1, keepdims=True)
    share = jnp.where(named, 1.0 / (1.0 + jnp.exp(both - 2.0 * chosen)), 0.0)
    high = share.astype(BF16).astype(F32)
    shares = (high + pltpu.roll(share - high, EXPERTS, 1)).astype(BF16)
    normed = (stream * scale * gain).astype(BF16)
    normed = jnp.concatenate([normed, shares], axis=1)
    picked = dot(picker, normed).astype(BF16)
    last = dot(last_picker, normed)
    for e in range(EXPERTS):
        rows_out[e] = picked[e * MAIN : (e + 1) * MAIN]
        last_out[e] = last[e : e + 1]

    def row_copies(step):
        to = (me + step) % count
        mine = place(me)
        return (
            pltpu.make_async_remote_copy(
                src_ref=rows_out.at[to // width],
                dst_ref=rows_in.at[mine],
                send_sem=row_send.at[step],
                recv_sem=row_recv.at[step],
                device_id={"expert": to},
                device_id_type=MESH,
            ),
            pltpu.make_async_remote_copy(
                src_ref=last_out.at[to // width],
                dst_ref=last_in.at[mine],
                send_sem=last_send.at[step],
                recv_sem=last_recv.at[step],
                device_id={"expert": to},
                device_id_type=MESH,
            ),
        )

    def over_copies(step):
        at = place((me - step + count) % count)
        return (
            pltpu.make_async_remote_copy(
                src_ref=rows_in.at[at, :, pl.ds(0, half)],
                dst_ref=rows_over.at[at],
                send_sem=over_send.at[step],
                recv_sem=over_recv.at[step],
                device_id={"sub": 1 - core},
                device_id_type=MESH,
            ),
            pltpu.make_async_remote_copy(
                src_ref=last_in.at[at, :, pl.ds(0, half)],
                dst_ref=last_over.at[at],
                send_sem=over_last_send.at[step],
                recv_sem=over_last_recv.at[step],
                device_id={"sub": 1 - core},
                device_id_type=MESH,
            ),
        )

    def start_rows(step, carry):
        for copy in row_copies(step):
            copy.start()
        return carry

    lax.fori_loop(1, count, start_rows, 0)
    rows_in[place(me)] = rows_out[holder]
    last_in[place(me)] = last_out[holder]
    for copy in over_copies(0):
        copy.start()

    def hand_on(step, carry):
        for copy in row_copies(step):
            copy.wait()
        for copy in over_copies(step):
            copy.start()
        return carry

    lax.fori_loop(1, count, hand_on, 0)

    span = EXPERTS * MAIN
    rows = EXPERTS * CAP
    wide = span + MAIN
    to_row = iota((rows, wide), 0)
    from_row = iota((rows, wide), 1)
    source = jnp.where(
        from_row < span, from_row + from_row // MAIN, (from_row - span) * CAP + MAIN
    )
    order = (to_row == source).astype(F32).astype(BF16)

    def lined_up(block, rows_ref, last_ref, lanes):
        at = pl.ds(block * EXPERTS, EXPERTS)
        main = rows_ref[at, :, lanes].reshape(span, -1)
        ends = [last_ref[block * EXPERTS + q, :, lanes] for q in range(EXPERTS)]
        ends.append(jnp.zeros((MAIN - EXPERTS, main.shape[1]), F32))
        tail = jnp.concatenate(ends, axis=0).astype(BF16)
        return dot(order, jnp.concatenate([main, tail], axis=0))

    def own_half(block, carry):
        slots[core, block] = lined_up(block, rows_in, last_in, slice(0, half)).astype(BF16)
        return carry

    lax.fori_loop(0, width, own_half, 0)

    def wait_over(step, carry):
        for copy in over_copies(step):
            copy.wait()
        return carry

    lax.fori_loop(0, count, wait_over, 0)

    def other_half(block, carry):
        slots[1 - core, block] = lined_up(block, rows_over, last_over, slice(0, half)).astype(BF16)
        return carry

    lax.fori_loop(0, width, other_half, 0)
    for load in loads:
        load.wait()

    columns = weights.shape[2]
    tile = min(256, columns)

    def block_rows(block, carry):
        share_rows = lined_up(block, rows_in, last_in, slice(half, half + LANES))
        share_lane = iota((rows, LANES), 1)
        wanted = (share_lane == holder) | (share_lane == holder + EXPERTS)
        slot_share = jnp.sum(jnp.where(wanted, share_rows, 0.0), axis=1, keepdims=True)

        def one_tile(index, inner):
            at = pl.ds(pl.multiple_of(index * tile, tile), tile)

            def product(side):
                return dot(slots[0, block], weights[side, 0:half, at]) + dot(
                    slots[1, block], weights[side, half : 2 * half, at]
                )

            gate = product(0)
            up = product(1)
            hidden_out[block, :, at] = (gate / (1.0 + jnp.exp(-gate)) * up * slot_share).astype(
                BF16
            )
            return inner

        lax.fori_loop(0, columns // tile, one_tile, 0)
        return carry

    lax.fori_loop(0, width, block_rows, 0)


def shards(
    stream_in,
    queries,
    kv_new,
    paged_key_value_cache,
    page_table,
    prefix_len,
    norm_gain,
    w_router,
    expert_ids,
    w_in,
):
    count = lax.axis_size("expert")
    width = count // EXPERTS
    tokens, half = stream_in.shape
    columns = w_in.shape[2]
    cache = paged_key_value_cache.reshape(2, -1, paged_key_value_cache.shape[-1])
    w_chunks = 6
    rows = EXPERTS * CAP
    vmem = pl.BlockSpec(memory_space=pltpu.VMEM)
    smem = pl.BlockSpec(memory_space=pltpu.SMEM)
    dma = pltpu.SemaphoreType.DMA
    stream, hidden = pl.pallas_call(
        lambda *refs: kernel(count, w_chunks, paged_key_value_cache.shape[2], *refs),
        name="moe_prefill",
        out_shape=(
            jax.ShapeDtypeStruct((tokens, half), BF16),
            jax.ShapeDtypeStruct((width, rows, columns), BF16),
        ),
        in_specs=[smem, smem] + [vmem] * 7 + [pl.BlockSpec(memory_space=pl.ANY)],
        out_specs=(vmem, vmem),
        scratch_shapes=[
            pltpu.VMEM(w_in.shape, BF16),
            pltpu.VMEM((count,) + cache.shape, BF16),
            pltpu.VMEM((2, tokens, LANES), F32),
            pltpu.VMEM((2, tokens, LANES), F32),
            pltpu.VMEM((EXPERTS, MAIN, half + LANES), BF16),
            pltpu.VMEM((EXPERTS, 1, half + LANES), F32),
            pltpu.VMEM((count, MAIN, half + LANES), BF16),
            pltpu.VMEM((count, 1, half + LANES), F32),
            pltpu.VMEM((count, MAIN, half), BF16),
            pltpu.VMEM((count, 1, half), F32),
            pltpu.VMEM((2, width, rows, half), BF16),
            dma((2, w_chunks)),
            dma((count,)),
            dma((count,)),
            dma,
            dma,
        ]
        + [dma((count,))] * 8,
        compiler_params=pltpu.CompilerParams(
            collective_id=0, has_side_effects=True, vmem_limit_bytes=67043328
        ),
    )(
        page_table,
        prefix_len,
        stream_in,
        queries,
        kv_new,
        cache,
        norm_gain.reshape(1, -1),
        w_router,
        expert_ids,
        w_in,
    )
    return stream, hidden.reshape(width * rows, columns)


def solution(mesh):
    placed = (
        P(("groups", "expert"), "sub"),
        P(("groups", "expert"), "sub"),
        P(None, ("groups", "expert"), "sub"),
        P(None, ("groups", "expert"), None, "sub"),
        P(("groups", "expert"), None),
        P(("groups", "expert")),
        P(),
        P(),
        P(("groups", "expert"), None),
        P(None, None, ("expert", "sub")),
    )
    return jax.shard_map(
        shards,
        mesh=mesh,
        in_specs=placed,
        out_specs=(P(("groups", "expert"), "sub"), P("groups", ("expert", "sub"))),
        check_vma=False,
    )
```

```python
import math

import jax
import jax.numpy as jnp
from jax import lax
from jax.experimental import pallas as pl
from jax.experimental.pallas import tpu as pltpu
from jax.sharding import PartitionSpec as P

HEAD_WIDTH = 128
EXPERTS = 8
CAP = 17
MAIN = 16
LANES = 128
F32 = jnp.float32
BF16 = jnp.bfloat16
MESH = pl.DeviceIdType.MESH


def dot(a, b):
    return jnp.dot(a, b, preferred_element_type=F32)


def iota(shape, dim):
    return lax.broadcasted_iota(jnp.int32, shape, dim)


def kernel(
    count,
    w_chunks,
    page_tokens,
    page_table,
    prefix_len,
    cache_hbm,
    queries_hbm,
    kv_new_hbm,
    stream_hbm,
    norm_gain_hbm,
    w_router_hbm,
    expert_ids_hbm,
    w_in,
    stream_result,
    hidden_result,
    cache,
    queries,
    kv_new,
    stream_in,
    norm_gain,
    w_router,
    expert_ids,
    stream_out,
    hidden_out,
    in_sem,
    stream_sem,
    hidden_sem,
    weights,
    kv_all,
    part,
    part_in,
    rows_out,
    last_out,
    rows_in,
    last_in,
    rows_over,
    last_over,
    slots,
    w_sem,
    page_send,
    page_recv,
    part_send,
    part_recv,
    row_send,
    row_recv,
    last_send,
    last_recv,
    over_send,
    over_recv,
    over_last_send,
    over_last_recv,
):
    me = lax.axis_index("expert")
    core = lax.axis_index("sub")
    width = count // EXPERTS
    half = stream_in.shape[1]
    tokens = stream_in.shape[0]
    holder = me // width

    def place(index):
        return (index % width) * EXPERTS + index // width

    pairs = (
        (cache_hbm, cache),
        (queries_hbm, queries),
        (kv_new_hbm, kv_new),
        (stream_hbm, stream_in),
        (norm_gain_hbm, norm_gain),
        (w_router_hbm, w_router),
        (expert_ids_hbm, expert_ids),
    )
    taken = [
        pltpu.make_async_copy(far, near, in_sem.at[index])
        for index, (far, near) in enumerate(pairs)
    ]
    for copy in taken:
        copy.start()
    barrier = pltpu.get_barrier_semaphore()

    def greet(step, carry):
        pl.semaphore_signal(
            barrier, inc=1, device_id={"expert": (me + step) % count}, device_id_type=MESH
        )
        return carry

    lax.fori_loop(1, count, greet, 0)
    pl.semaphore_signal(barrier, inc=1, device_id={"sub": 1 - core}, device_id_type=MESH)

    depth = weights.shape[1] // w_chunks
    loads = []
    for chunk in range(w_chunks):
        for side in range(2):
            span = pl.ds(chunk * depth, depth)
            load = pltpu.make_async_copy(
                w_in.at[side, span], weights.at[side, span], w_sem.at[side, chunk]
            )
            load.start()
            loads.append(load)

    taken[0].wait()
    pl.semaphore_wait(barrier, count)

    def page_copy(step):
        return pltpu.make_async_remote_copy(
            src_ref=cache,
            dst_ref=kv_all.at[me],
            send_sem=page_send.at[step],
            recv_sem=page_recv.at[step],
            device_id={"expert": (me + step) % count},
            device_id_type=MESH,
        )

    def start_pages(step, carry):
        page_copy(step).start()
        return carry

    lax.fori_loop(1, count, start_pages, 0)
    kv_all[me] = cache[...]
    for copy in taken[1:]:
        copy.wait()

    shard_pages = cache.shape[1]
    shard_rows = shard_pages * page_tokens
    page_rows = kv_all.shape[0] * shard_rows
    table_pages = page_table.shape[1]
    tokens_page = page_tokens
    key_heads = kv_new.shape[2] // HEAD_WIDTH
    grouped = half // HEAD_WIDTH // key_heads
    scaling = 1.0 / math.sqrt(HEAD_WIDTH)
    flat = ((1,), (1,)), ((), ())
    stacked = tokens * grouped
    causal = iota((stacked, tokens), 1) <= iota((stacked, tokens), 0) % tokens
    asked = []
    own_scores = []
    for head in range(key_heads):
        lanes = slice(head * HEAD_WIDTH, (head + 1) * HEAD_WIDTH)
        query = jnp.concatenate(
            [
                queries[:, (head * grouped + g) * HEAD_WIDTH : (head * grouped + g + 1) * HEAD_WIDTH]
                for g in range(grouped)
            ],
            axis=0,
        )
        asked.append(query)
        score = lax.dot_general(query, kv_new[0, :, lanes], flat, preferred_element_type=F32)
        own_scores.append(jnp.where(causal, score * scaling, -1e30))

    row_at = iota((1, page_rows), 1)
    page_at = row_at // tokens_page

    def find(j, found):
        return jnp.where(page_at == page_table[0, j], j * tokens_page, found)

    never = jnp.full((1, page_rows), 1 << 29, jnp.int32)
    position = lax.fori_loop(0, table_pages, find, never) + row_at % tokens_page
    alive = position < prefix_len[0]

    def cached(kind, lanes):
        pages = [kv_all[:, kind, p, :, lanes].astype(F32) for p in range(shard_pages)]
        joined = jnp.concatenate(pages, axis=1)
        return joined.reshape(page_rows, HEAD_WIDTH).astype(BF16)

    def wait_pages(step, carry):
        page_copy(step).wait()
        return carry

    lax.fori_loop(1, count, wait_pages, 0)

    for head in range(key_heads):
        lanes = slice(head * HEAD_WIDTH, (head + 1) * HEAD_WIDTH)
        keys = cached(0, lanes)
        values = cached(1, lanes)
        old = lax.dot_general(asked[head], keys, flat, preferred_element_type=F32) * scaling
        old = jnp.where(alive, old, -1e30)
        new = own_scores[head]
        largest = jnp.maximum(
            jnp.max(old, axis=1, keepdims=True), jnp.max(new, axis=1, keepdims=True)
        )
        old = jnp.exp(old - largest)
        new = jnp.exp(new - largest)
        total = jnp.sum(old, axis=1, keepdims=True) + jnp.sum(new, axis=1, keepdims=True)
        mixed = dot((old / total).astype(BF16), values)
        mixed = mixed + dot((new / total).astype(BF16), kv_new[1, :, lanes])
        mixed = mixed.astype(BF16).astype(F32)
        for g in range(grouped):
            at = slice((head * grouped + g) * HEAD_WIDTH, (head * grouped + g + 1) * HEAD_WIDTH)
            stream_out[:, at] = (
                stream_in[:, at].astype(F32) + mixed[g * tokens : (g + 1) * tokens]
            ).astype(BF16)

    keep = pltpu.make_async_copy(stream_out, stream_result, stream_sem)
    keep.start()
    stream = stream_out[...].astype(F32)
    first = pl.multiple_of(core * half, LANES)
    gain = norm_gain[:, pl.ds(first, half)]
    squares = jnp.sum(stream * stream, axis=1, keepdims=True)
    raw = lax.dot_general(
        (stream * gain).astype(BF16),
        w_router[:, pl.ds(first, half)],
        flat,
        preferred_element_type=F32,
    )
    part[0] = jnp.zeros((tokens, LANES), F32)
    part[0, :, 0:EXPERTS] = raw
    part[1] = jnp.broadcast_to(squares, (tokens, LANES))
    swap = pltpu.make_async_remote_copy(
        src_ref=part,
        dst_ref=part_in,
        send_sem=part_send,
        recv_sem=part_recv,
        device_id={"sub": 1 - core},
        device_id_type=MESH,
    )
    swap.start()

    name = iota((EXPERTS, tokens), 0)
    named = (expert_ids[0:1, :] == name) | (expert_ids[1:2, :] == name)
    named_f = named.astype(F32)
    before = (iota((tokens, tokens), 0) < iota((tokens, tokens), 1)).astype(F32).astype(BF16)
    rank = jnp.where(named, dot(named_f.astype(BF16), before), -1.0)
    spot = (iota((EXPERTS, LANES), 0) == iota((EXPERTS, LANES), 1)).astype(F32).astype(BF16)
    turn = ((0,), (0,)), ((), ())
    hot = lax.dot_general(named_f.astype(BF16), spot, turn, preferred_element_type=F32)
    slot = iota((MAIN, tokens), 0).astype(F32)
    picker = jnp.concatenate(
        [
            (jnp.broadcast_to(rank[e : e + 1], (MAIN, tokens)) == slot).astype(F32)
            for e in range(EXPERTS)
        ],
        axis=0,
    ).astype(BF16)
    last_picker = (rank == float(MAIN)).astype(F32).astype(BF16)

    swap.wait()
    scale = lax.rsqrt((part[1] + part_in[1])[:, 0:1] / (2 * half) + 1e-05)
    logits = (part[0] + part_in[0]) * scale
    chosen = logits * hot
    both = jnp.sum(chosen, axis=1, keepdims=True)
    share = jnp.where(hot > 0.5, 1.0 / (1.0 + jnp.exp(both - 2.0 * chosen)), 0.0)
    high = share.astype(BF16).astype(F32)
    shares = (high + pltpu.roll(share - high, EXPERTS, 1)).astype(BF16)
    normed = (stream * scale * gain).astype(BF16)
    normed = jnp.concatenate([normed, shares], axis=1)
    picked = dot(picker, normed).astype(BF16)
    last = dot(last_picker, normed)
    for e in range(EXPERTS):
        rows_out[e] = picked[e * MAIN : (e + 1) * MAIN]
        last_out[e] = last[e : e + 1]

    def row_copies(step):
        to = (me + step) % count
        mine = place(me)
        return (
            pltpu.make_async_remote_copy(
                src_ref=rows_out.at[to // width],
                dst_ref=rows_in.at[mine],
                send_sem=row_send.at[step],
                recv_sem=row_recv.at[step],
                device_id={"expert": to},
                device_id_type=MESH,
            ),
            pltpu.make_async_remote_copy(
                src_ref=last_out.at[to // width],
                dst_ref=last_in.at[mine],
                send_sem=last_send.at[step],
                recv_sem=last_recv.at[step],
                device_id={"expert": to},
                device_id_type=MESH,
            ),
        )

    def over_copies(step):
        at = place((me - step + count) % count)
        return (
            pltpu.make_async_remote_copy(
                src_ref=rows_in.at[at, :, pl.ds(0, half)],
                dst_ref=rows_over.at[at],
                send_sem=over_send.at[step],
                recv_sem=over_recv.at[step],
                device_id={"sub": 1 - core},
                device_id_type=MESH,
            ),
            pltpu.make_async_remote_copy(
                src_ref=last_in.at[at, :, pl.ds(0, half)],
                dst_ref=last_over.at[at],
                send_sem=over_last_send.at[step],
                recv_sem=over_last_recv.at[step],
                device_id={"sub": 1 - core},
                device_id_type=MESH,
            ),
        )

    def start_rows(step, carry):
        for copy in row_copies(step):
            copy.start()
        return carry

    lax.fori_loop(1, count, start_rows, 0)
    rows_in[place(me)] = rows_out[holder]
    last_in[place(me)] = last_out[holder]
    for copy in over_copies(0):
        copy.start()

    def hand_on(step, carry):
        for copy in row_copies(step):
            copy.wait()
        for copy in over_copies(step):
            copy.start()
        return carry

    lax.fori_loop(1, count, hand_on, 0)

    span = EXPERTS * MAIN
    rows = EXPERTS * CAP
    wide = span + MAIN
    to_row = iota((rows, wide), 0)
    from_row = iota((rows, wide), 1)
    source = jnp.where(
        from_row < span, from_row + from_row // MAIN, (from_row - span) * CAP + MAIN
    )
    order = (to_row == source).astype(F32).astype(BF16)

    def lined_up(block, rows_ref, last_ref, lanes):
        at = pl.ds(block * EXPERTS, EXPERTS)
        main = rows_ref[at, :, lanes].reshape(span, -1)
        ends = [last_ref[block * EXPERTS + q, :, lanes] for q in range(EXPERTS)]
        ends.append(jnp.zeros((MAIN - EXPERTS, main.shape[1]), F32))
        tail = jnp.concatenate(ends, axis=0).astype(BF16)
        return dot(order, jnp.concatenate([main, tail], axis=0))

    def own_half(block, carry):
        slots[core, block] = lined_up(block, rows_in, last_in, slice(0, half)).astype(BF16)
        return carry

    lax.fori_loop(0, width, own_half, 0)

    def wait_over(step, carry):
        for copy in over_copies(step):
            copy.wait()
        return carry

    lax.fori_loop(0, count, wait_over, 0)

    def other_half(block, carry):
        slots[1 - core, block] = lined_up(block, rows_over, last_over, slice(0, half)).astype(BF16)
        return carry

    lax.fori_loop(0, width, other_half, 0)
    for load in loads:
        load.wait()

    columns = weights.shape[2]
    tile = min(1024, columns)

    tiles = columns // tile

    def tile_copy(block, index):
        at = pl.ds(pl.multiple_of(index * tile, tile), tile)
        return pltpu.make_async_copy(
            hidden_out.at[block, :, at],
            hidden_result.at[block, :, at],
            hidden_sem.at[block * tiles + index],
        )

    def block_rows(block, carry):
        share_rows = lined_up(block, rows_in, last_in, slice(half, half + LANES))
        share_lane = iota((rows, LANES), 1)
        wanted = (share_lane == holder) | (share_lane == holder + EXPERTS)
        slot_share = jnp.sum(jnp.where(wanted, share_rows, 0.0), axis=1, keepdims=True)

        def one_tile(index, inner):
            at = pl.ds(pl.multiple_of(index * tile, tile), tile)

            def product(side):
                return dot(slots[0, block], weights[side, 0:half, at]) + dot(
                    slots[1, block], weights[side, half : 2 * half, at]
                )

            gate = product(0)
            up = product(1)
            hidden_out[block, :, at] = (gate / (1.0 + jnp.exp(-gate)) * up * slot_share).astype(
                BF16
            )
            tile_copy(block, index).start()
            return inner

        lax.fori_loop(0, columns // tile, one_tile, 0)
        return carry

    lax.fori_loop(0, width, block_rows, 0)

    def settle(step, carry):
        tile_copy(step // tiles, step % tiles).wait()
        return carry

    lax.fori_loop(0, width * tiles, settle, 0)
    keep.wait()


def pass_on(cuts, stream, hidden, stream_out, hidden_out, stream_in, hidden_in, ins, outs):
    width = hidden.shape[2] // cuts
    into = [pltpu.make_async_copy(stream, stream_in, ins.at[cuts])]
    out = [pltpu.make_async_copy(stream_in, stream_out, outs.at[cuts])]
    for cut in range(cuts):
        at = (slice(None), slice(None), pl.ds(cut * width, width))
        into.append(pltpu.make_async_copy(hidden.at[at], hidden_in.at[at], ins.at[cut]))
        out.append(pltpu.make_async_copy(hidden_in.at[at], hidden_out.at[at], outs.at[cut]))
    for copy in into:
        copy.start()
    for arrived, leaving in zip(into, out):
        arrived.wait()
        leaving.start()
    for copy in out:
        copy.wait()


def shards(
    stream_in,
    queries,
    kv_new,
    paged_key_value_cache,
    page_table,
    prefix_len,
    norm_gain,
    w_router,
    expert_ids,
    w_in,
):
    count = lax.axis_size("expert")
    width = count // EXPERTS
    tokens, half = stream_in.shape
    columns = w_in.shape[2]
    cache = paged_key_value_cache
    w_chunks = 6
    rows = EXPERTS * CAP
    hbm = pl.BlockSpec(memory_space=pl.ANY)
    gain = norm_gain.reshape(1, -1)
    near = (cache, queries, kv_new, stream_in, gain, w_router.T, expert_ids.T)
    smem = pl.BlockSpec(memory_space=pltpu.SMEM)
    dma = pltpu.SemaphoreType.DMA
    stream, hidden = pl.pallas_call(
        lambda *refs: kernel(count, w_chunks, paged_key_value_cache.shape[2], *refs),
        name="moe_prefill",
        out_shape=(
            jax.ShapeDtypeStruct((tokens, half), BF16),
            jax.ShapeDtypeStruct((width, rows, columns), BF16),
        ),
        in_specs=[smem, smem] + [hbm] * 8,
        out_specs=(hbm, hbm),
        scratch_shapes=[pltpu.VMEM(array.shape, array.dtype) for array in near]
        + [
            pltpu.VMEM((tokens, half), BF16),
            pltpu.VMEM((width, rows, columns), BF16),
            dma((len(near),)),
            dma,
            dma((width * max(columns // 1024, 1),)),
            pltpu.VMEM(w_in.shape, BF16),
            pltpu.VMEM((count,) + cache.shape, BF16),
            pltpu.VMEM((2, tokens, LANES), F32),
            pltpu.VMEM((2, tokens, LANES), F32),
            pltpu.VMEM((EXPERTS, MAIN, half + LANES), BF16),
            pltpu.VMEM((EXPERTS, 1, half + LANES), F32),
            pltpu.VMEM((count, MAIN, half + LANES), BF16),
            pltpu.VMEM((count, 1, half + LANES), F32),
            pltpu.VMEM((count, MAIN, half), BF16),
            pltpu.VMEM((count, 1, half), F32),
            pltpu.VMEM((2, width, rows, half), BF16),
            dma((2, w_chunks)),
            dma((count,)),
            dma((count,)),
            dma,
            dma,
        ]
        + [dma((count,))] * 8,
        compiler_params=pltpu.CompilerParams(
            collective_id=0, has_side_effects=True, vmem_limit_bytes=58 << 20
        ),
    )(
        page_table,
        prefix_len,
        *near,
        w_in,
    )
    cuts = 4 if columns % (4 * LANES) == 0 else 1
    stream, hidden = pl.pallas_call(
        lambda *refs: pass_on(cuts, *refs),
        name="pass_on",
        out_shape=(
            jax.ShapeDtypeStruct(stream.shape, BF16),
            jax.ShapeDtypeStruct(hidden.shape, BF16),
        ),
        in_specs=[hbm, hbm],
        out_specs=(hbm, hbm),
        scratch_shapes=[
            pltpu.VMEM(stream.shape, BF16),
            pltpu.VMEM(hidden.shape, BF16),
            dma((cuts + 1,)),
            dma((cuts + 1,)),
        ],
    )(stream, hidden)
    return stream, hidden.reshape(width * rows, columns)


def solution(mesh):
    placed = (
        P(("groups", "expert"), "sub"),
        P(("groups", "expert"), "sub"),
        P(None, ("groups", "expert"), "sub"),
        P(None, ("groups", "expert"), None, "sub"),
        P(("groups", "expert"), None),
        P(("groups", "expert")),
        P(),
        P(),
        P(("groups", "expert"), None),
        P(None, None, ("expert", "sub")),
    )
    return jax.shard_map(
        shards,
        mesh=mesh,
        in_specs=placed,
        out_specs=(P(("groups", "expert"), "sub"), P("groups", ("expert", "sub"))),
        check_vma=False,
    )
```
